32 devices in a mesh: dp: 2 (over x), fsdp: 4 (over z), tensor: 4 (over y, core).
Axes of the slice: x: 2, y: 2, z: 4, core: 2. Of those that a mesh axis runs over, the one named last changes fastest.
Arguments:
- grads: bfloat16 [2, 4, 16, 53248], P('dp', 'fsdp', None, 'tensor'), may hold values from -64 to 64, as said below
- params: bfloat16 [16, 53248], P('fsdp', 'tensor'), may hold values from -0.119628906 to 0.119628906
- moment_norm: bfloat16 [16, 53248], P('fsdp', 'tensor'), may hold values from -1 to 1
- moment_scale: float32 [16, 416], P('fsdp', 'tensor'), may hold values from 0.05 to 0.5
- second_norm: bfloat16 [16, 53248], P('fsdp', 'tensor'), may hold values from 0.049804688 to 1
- second_rows: float32 [16], P('fsdp'), may hold values from 0.01 to 0.1
- second_cols: float32 [53248], P('tensor'), may hold values from 0.01 to 0.1
Outputs:
- new_params: bfloat16 [16, 53248], P(None, 'tensor')
- next_moment: bfloat16 [16, 53248], P('fsdp', 'tensor')
- next_moment_scale: float32 [16, 416], P('fsdp', 'tensor')
- next_second: bfloat16 [16, 53248], P('fsdp', 'tensor')
- next_second_rows: float32 [16], P('fsdp')
- next_second_cols: float32 [53248], P('tensor')
The draws below stay inside these ranges and needn't reach their ends.
Inputs may be any that keep to these rules, and one draw needn't show every extreme that they name: `grads`: partial gradients; magnitudes are at most 64.
All inputs are finite; a program needn't handle non-finite values. Where the reference program divides by a largest or mean magnitude, that divisor is 1e-20 or more.
Results may differ from the reference program's by a relative error of at most 0.0004.
Values may be sent and summed in bfloat16 or wider, within the bound.
No kernel may reach another device: no remote copies, remote signals or barrier semaphores. Data moves between devices by JAX's collectives and lax.ppermute only.
A program may use at most 64 MiB of HBM per device.

```python
import math
import jax
import jax.numpy as jnp
from jax import lax

F = 53248
ROWS_DEV = 4
BLOCK = 128
STEP = 10
ROWS = 16
N_DP = 2
N_FSDP = 4


def draw_grads(key, part):
    key_noise = jax.random.fold_in(key, 11)
    key_rows = jax.random.fold_in(key, 12)
    key_cols = jax.random.fold_in(key, 13)
    key_pairs = jax.random.fold_in(key, 14)
    noise = jnp.clip(jax.random.normal(key_noise, (N_DP, N_FSDP, ROWS, F), jnp.float32), -4.0, 4.0)
    row_index = jnp.arange(ROWS, dtype=jnp.float32)
    col_index = jnp.arange(F, dtype=jnp.float32)
    row_scale = 10.0 ** (row_index / ROWS) * jax.random.uniform(key_rows, (ROWS,), jnp.float32, 0.7, 1.4)
    col_scale = 3.0 ** (col_index / F) * jnp.exp(jax.random.uniform(key_cols, (F,), jnp.float32, 0.0, math.log(10.0)))
    pairing = jax.random.permutation(key_pairs, N_FSDP)
    owner = jnp.arange(ROWS) // ROWS_DEV
    boost = jnp.where(owner[None, :] == pairing[:, None], 4.0, 1.0).astype(jnp.float32)
    values = 0.03 * noise * row_scale[None, None, :, None] * col_scale[None, None, None, :] * boost[None, :, :, None]
    return jnp.clip(values, -64.0, 64.0).astype(jnp.bfloat16)


def steps_of(rng, extent, cuts, smallest, largest):
    def one(dim, blocks):
        heights = jax.random.uniform(jax.random.fold_in(jax.random.fold_in(rng, 6), dim), (blocks,), jnp.float32, smallest / len(cuts), largest / len(cuts))
        return jnp.repeat(jnp.exp(heights), extent[dim] // blocks).reshape((-1,) + (1,) * (len(extent) - dim - 1))

    gain = one(*cuts[0])
    for cut in cuts[1:]:
        gain = gain * one(*cut)
    return gain


def centred(key, dims, deviation, most, shards=(), kind=jnp.bfloat16):
    factor_of = steps_of(key, dims, shards, -0.22, 0.18) if shards else 1.0
    entries = jax.random.normal(key, dims, jnp.float32) * deviation * factor_of
    return jnp.minimum(jnp.maximum(entries, -most), most).astype(kind)


def setup_inputs(seed: int = 0) -> dict:
    arg_keys = jax.random.split(jax.random.key(seed), 8)
    return {
        "grads": draw_grads(jax.random.fold_in(arg_keys[7], 71), 0),
        "params": centred(arg_keys[1], (ROWS, F), 0.02, 0.119628906, ((0, 4), (1, 4))),
        "moment_norm": jnp.clip(jax.random.uniform(arg_keys[2], (ROWS, F), jnp.float32, -1.0, 1.0) * steps_of(arg_keys[2], (ROWS, F), ((0, 4), (1, 4)), -0.4, 0.0), -1.0, 1.0).astype(jnp.bfloat16),
        "moment_scale": jnp.clip(jnp.exp(math.log(0.5) - 2.3025851 * jax.random.uniform(arg_keys[3], (ROWS, F // BLOCK), jnp.float32) ** steps_of(arg_keys[3], (ROWS, F // BLOCK), ((0, 4), (1, 4)), -0.2, 0.2)), 0.05, 0.5),
        "second_norm": jnp.clip(0.049804688 + 0.9501953 * jax.random.uniform(arg_keys[4], (ROWS, F), jnp.float32) ** steps_of(arg_keys[4], (ROWS, F), ((0, 4), (1, 4)), -0.2, 0.2), 0.049804688, 1.0).astype(jnp.bfloat16),
        "second_rows": jnp.clip(jnp.exp(math.log(0.1) - 2.3025851 * jax.random.uniform(arg_keys[5], (ROWS,), jnp.float32) ** steps_of(arg_keys[5], (ROWS,), ((0, 4),), -0.2, 0.2)), 0.01, 0.1),
        "second_cols": jnp.clip(jnp.exp(math.log(0.1) - 2.3025851 * jax.random.uniform(arg_keys[6], (F,), jnp.float32) ** steps_of(arg_keys[6], (F,), ((0, 4),), -0.2, 0.2)), 0.01, 0.1),
    }


beta_one = 0.9
beta_two = 0.95
learn_rate = 0.01
decay_weight = 0.1
clip_rms = 0.3

def reference(grads, params, moment_norm, moment_scale, second_norm, second_rows, second_cols):
    summed = lax.optimization_barrier(jnp.sum(grads, axis=(0, 1), dtype=jnp.float32))
    total = jnp.sum(summed * summed)
    limit = clip_rms * math.sqrt(ROWS * F)
    factor = jnp.minimum(jnp.float32(1.0), limit / jnp.sqrt(total + 1e-06))
    clipped = factor * summed
    blocks = F // BLOCK
    first_old = (moment_norm.astype(jnp.float32).reshape(ROWS, blocks, BLOCK) * moment_scale[:, :, None]).reshape(ROWS, F)
    first = beta_one * first_old + (1.0 - beta_one) * clipped
    second_old = second_norm.astype(jnp.float32) * jnp.minimum(second_rows[:, None], second_cols[None, :])
    second = beta_two * second_old + (1.0 - beta_two) * clipped * clipped
    plain = params.astype(jnp.float32)
    ratio = first / (1.0 - beta_one ** STEP) / (jnp.sqrt(second / (1.0 - beta_two ** STEP)) + 1e-08)
    new_params = (plain - learn_rate * (ratio + decay_weight * plain)).astype(jnp.bfloat16)
    grouped = first.reshape(ROWS, blocks, BLOCK)
    next_moment_scale = lax.optimization_barrier(jnp.max(jnp.abs(grouped), axis=2))
    next_moment = (grouped / (next_moment_scale[:, :, None] + 1e-06)).reshape(ROWS, F).astype(jnp.bfloat16)
    next_second_rows = lax.optimization_barrier(jnp.max(second, axis=1))
    next_second_cols = lax.optimization_barrier(jnp.max(second, axis=0))
    next_second = (second / jnp.minimum(next_second_rows[:, None], next_second_cols[None, :])).astype(jnp.bfloat16)
    return (new_params, next_moment, next_moment_scale, next_second, next_second_rows, next_second_cols)
```

```python
import math

import jax
import jax.numpy as jnp
from jax import lax
from jax.sharding import PartitionSpec as P

BLOCK = 128
STEP = 10
DIRECT_LIMIT = 8


beta_one = 0.9
beta_two = 0.95
learn_rate = 0.01
decay_weight = 0.1
clip_rms = 0.3


def pairs(count, step):
    return [(i, i ^ step) for i in range(count)]


def owned_sum(grads, dp_count, fsdp_count):
    rows = grads.shape[0] // fsdp_count
    cols = grads.shape[1] // dp_count
    count = dp_count * fsdp_count
    me = lax.axis_index("dp") * fsdp_count + lax.axis_index("fsdp")

    def block(owner):
        return lax.dynamic_slice(grads, (owner % fsdp_count * rows, owner // fsdp_count * cols), (rows, cols))

    if count <= DIRECT_LIMIT and count & (count - 1) == 0:
        out = block(me).astype(jnp.float32)
        for step in range(1, count):
            got = lax.ppermute(block(me ^ step), ("dp", "fsdp"), pairs(count, step))
            out = out + got.astype(jnp.float32)
        return out
    stacked = grads.reshape(fsdp_count, rows, dp_count, cols).transpose(2, 0, 1, 3).reshape(count, rows, cols)
    return jnp.sum(lax.all_to_all(stacked, ("dp", "fsdp"), 0, 0, tiled=True), axis=0, dtype=jnp.float32)


def joined_columns(part, dp_count):
    if dp_count == 2:
        other = lax.ppermute(part, "dp", pairs(2, 1))
        first = lax.axis_index("dp") == 0
        return jnp.concatenate([jnp.where(first, part, other), jnp.where(first, other, part)], axis=1)
    return lax.all_gather(part, "dp", axis=1, tiled=True)


def sum_everywhere(value, axes, count):
    sent = jnp.broadcast_to(value, (count, 1, BLOCK))
    return jnp.sum(lax.all_to_all(sent, axes, 0, 0, tiled=True)[:, 0, 0])


def max_over(value, axis, count):
    if count <= DIRECT_LIMIT and count & (count - 1) == 0:
        out = value
        for step in range(1, count):
            out = jnp.maximum(out, lax.ppermute(value, axis, pairs(count, step)))
        return out
    return lax.pmax(value, axis)


def gathered_rows(rows, axis, count):
    if count <= DIRECT_LIMIT and count & (count - 1) == 0:
        blocks = [rows] + [lax.ppermute(rows, axis, pairs(count, step)) for step in range(1, count)]
        me = lax.axis_index(axis)
        stacked = jnp.stack(blocks)
        return jnp.concatenate([lax.dynamic_index_in_dim(stacked, me ^ j, 0, False) for j in range(count)], axis=0)
    return lax.all_gather(rows, axis, axis=0, tiled=True)


def on_device(grads, params, moment_norm, moment_scale, second_norm, second_rows, second_cols):
    dp_count = lax.axis_size("dp")
    fsdp_count = lax.axis_size("fsdp")
    tensor_count = lax.axis_size("tensor")
    own_rows, own_cols = params.shape
    limit = clip_rms * math.sqrt(own_rows * fsdp_count * own_cols * tensor_count)
    part = owned_sum(grads[0, 0], dp_count, fsdp_count)
    summed = joined_columns(part, dp_count)
    total = sum_everywhere(jnp.sum(part * part), ("dp", "fsdp", "tensor"), dp_count * fsdp_count * tensor_count)
    factor = jnp.minimum(jnp.float32(1.0), limit / jnp.sqrt(total + 1e-06))
    clipped = factor * summed
    blocks = own_cols // BLOCK
    first_old = (
        moment_norm.astype(jnp.float32).reshape(own_rows, blocks, BLOCK) * moment_scale[:, :, None]
    ).reshape(own_rows, own_cols)
    first = beta_one * first_old + (1.0 - beta_one) * clipped
    second_old = second_norm.astype(jnp.float32) * jnp.minimum(
        second_rows[:, None], second_cols[None, :]
    )
    second = beta_two * second_old + (1.0 - beta_two) * clipped * clipped
    row_peak = max_over(jnp.max(second, axis=1), "tensor", tensor_count)
    col_peak = max_over(jnp.max(second, axis=0), "fsdp", fsdp_count)
    plain = params.astype(jnp.float32)
    ratio = first / (1.0 - beta_one**STEP) / (jnp.sqrt(second / (1.0 - beta_two**STEP)) + 1e-08)
    updated = (plain - learn_rate * (ratio + decay_weight * plain)).astype(jnp.bfloat16)
    new_params = gathered_rows(updated, "fsdp", fsdp_count)
    grouped = first.reshape(own_rows, blocks, BLOCK)
    next_moment_scale = jnp.max(jnp.abs(grouped), axis=2)
    next_moment = (
        (grouped / (next_moment_scale[:, :, None] + 1e-06))
        .reshape(own_rows, own_cols)
        .astype(jnp.bfloat16)
    )
    next_second = (second / jnp.minimum(row_peak[:, None], col_peak[None, :])).astype(jnp.bfloat16)
    return (new_params, next_moment, next_moment_scale, next_second, row_peak, col_peak)


def solution(mesh):
    in_specs = (
        P("dp", "fsdp", None, "tensor"),
        P("fsdp", "tensor"),
        P("fsdp", "tensor"),
        P("fsdp", "tensor"),
        P("fsdp", "tensor"),
        P("fsdp"),
        P("tensor"),
    )
    out_specs = (
        P(None, "tensor"),
        P("fsdp", "tensor"),
        P("fsdp", "tensor"),
        P("fsdp", "tensor"),
        P("fsdp"),
        P("tensor"),
    )
    return jax.shard_map(
        on_device, mesh=mesh, in_specs=in_specs, out_specs=out_specs, check_vma=False
    )
```
